256 devices in a mesh: groups: 4 (over y, x), tile: 64 (over z, core).
Axes of the slice: x: 2, y: 2, z: 32, core: 2. Of those that a mesh axis runs over, the one named last changes fastest.
The devices are a block of a 4x8x32 slice.
Arguments:
- self_query: bfloat16 [32768, 4096], P(('groups', 'tile')), parts along dimension 0, may hold values from -110 to 110
- self_key: bfloat16 [32768, 4096], P(('groups', 'tile')), parts along dimension 0, may hold values from -6 to 6
- self_value: bfloat16 [32768, 4096], P(('groups', 'tile')), parts along dimension 0, may hold values from -24 to 24
- cross_query: bfloat16 [32768, 4096], P(('groups', 'tile')), parts along dimension 0, may hold values from -110 to 110
- text_key: bfloat16 [1024, 4096], P(('groups', 'tile')), parts along dimension 0, may hold values from -6 to 6
- text_value: bfloat16 [1024, 4096], P(('groups', 'tile')), parts along dimension 0, may hold values from -24 to 24
- timestep: int32 [1], replicated, may hold values from 0 to 49
- gate_table: bfloat16 [50, 4096], replicated, may hold values from 0.5 to 2
Outputs:
- mixed: bfloat16 [32768, 4096], P(('groups', 'tile')), parts along dimension 0
The draws below stay inside these ranges and needn't reach their ends.
There are 4 independent parts, one for each index of `groups`. The reference program is written for one: setup_inputs(seed, part) draws one part's arguments, and reference() takes and returns one part's arrays. A program takes and returns all parts, laid end to end along the dimension named above; an argument that names none is the same for every part. Nothing has to cross between parts.
All inputs are finite; a program needn't handle non-finite values.
Results may differ from the reference program's by a relative error of at most 0.0032.
Values may be sent and summed in bfloat16 or wider, within the bound.
A program may use at most 64 MiB of HBM per device.

```python
import math
import jax
import jax.numpy as jnp
from jax import lax

HEADS = 32
HEAD_DIM = 128
WIDTH = 4096
TOK_DEV = 128
RADIUS = 2
TEXT = 256
STEPS = 50
TILES = 64
TOKENS = 8192


def paired_draw(key, label, query_count, key_count):
    folded = jax.random.fold_in(key, label)
    width = HEADS * HEAD_DIM
    key_draw = 1.5 * jax.random.truncated_normal(jax.random.fold_in(folded, 1), -4.0, 4.0, (key_count, width), jnp.float32)
    query_draw = 1.5 * jax.random.truncated_normal(jax.random.fold_in(folded, 2), -4.0, 4.0, (query_count, width), jnp.float32)
    return (query_draw, key_draw)


def draw_self_query(key, part):
    return paired_draw(key, 11, TOKENS, TOKENS)[0].astype(jnp.bfloat16)


def draw_self_key(key, part):
    return paired_draw(key, 11, TOKENS, TOKENS)[1].astype(jnp.bfloat16)


def draw_cross_query(key, part):
    return paired_draw(key, 23, TOKENS, TEXT)[0].astype(jnp.bfloat16)


def draw_text_key(key, part):
    return paired_draw(key, 23, TOKENS, TEXT)[1].astype(jnp.bfloat16)


def steps_of(own_key, extent, pieces, smallest, high):
    factor_of, own = 1.0, jax.random.fold_in(own_key, 6)
    for dim, parts in pieces:
        steps = jnp.exp(jax.random.uniform(jax.random.fold_in(own, dim), (parts,), jnp.float32, smallest / len(pieces), high / len(pieces)))
        factor_of = factor_of * jnp.repeat(steps, extent[dim] // parts).reshape([-1 if axis == dim else 1 for axis in range(len(extent))])
    return factor_of


def noise(own_key, extent, scale, limit, pieces=(), kind=jnp.bfloat16):
    array = jax.random.normal(own_key, extent, jnp.float32) * scale
    if len(pieces) > 0:
        array = steps_of(own_key, extent, pieces, -0.22, 0.18) * array
    return jnp.clip(array, min=-limit, max=limit).astype(kind)


def setup_inputs(seed: int = 0, part: int = 0) -> dict:
    key_of = jax.random.split(jax.random.key(seed), 9)
    part_keys = jax.random.split(jax.random.fold_in(key_of[8], part), 9)
    self_query = draw_self_query(jax.random.fold_in(jax.random.fold_in(key_of[8], part), 71), part)
    self_key = draw_self_key(jax.random.fold_in(jax.random.fold_in(key_of[8], part), 71), part)
    self_value = noise(part_keys[2], (TOKENS, WIDTH), 4.0, 24.0, ((0, 64),))
    cross_query = draw_cross_query(jax.random.fold_in(jax.random.fold_in(key_of[8], part), 71), part)
    text_key = draw_text_key(jax.random.fold_in(jax.random.fold_in(key_of[8], part), 71), part)
    text_value = noise(part_keys[5], (TEXT, WIDTH), 4.0, 24.0, ((0, 64),))
    timestep = jax.random.randint(key_of[6], (1,), 0, STEPS).astype(jnp.int32)
    gate_table = jnp.clip(jax.random.uniform(key_of[7], (STEPS, WIDTH), jnp.float32, 0.5, 2.0), 0.5, 2.0).astype(jnp.bfloat16)
    return dict(self_query=self_query, self_key=self_key, self_value=self_value, cross_query=cross_query, text_key=text_key, text_value=text_value, timestep=timestep, gate_table=gate_table)


def window_attention(queries, key_block, value_block, usable):
    score_scale = 1.0 / math.sqrt(HEAD_DIM)
    scores = jnp.einsum('qhd,khd->hqk', queries, key_block) * score_scale
    masked = jnp.where(usable[None, None, :], scores, -1e+30)
    maxima = lax.optimization_barrier(jnp.max(masked, axis=2, keepdims=True))
    weights = jnp.where(usable[None, None, :], jnp.exp(masked - maxima), 0.0)
    totals = lax.optimization_barrier(jnp.sum(weights, axis=2, keepdims=True))
    rounded = lax.optimization_barrier(weights.astype(jnp.bfloat16)).astype(jnp.float32)
    summed = jnp.einsum('hqk,khd->qhd', rounded, value_block)
    return summed / jnp.transpose(totals, (1, 0, 2))

def reference(self_query, self_key, self_value, cross_query, text_key, text_value, timestep, gate_table):
    width = HEADS * HEAD_DIM
    window_span = 2 * RADIUS + 1
    margin = jnp.zeros((RADIUS * TOK_DEV, width), jnp.bfloat16)
    padded_keys = jnp.concatenate([margin, self_key, margin], axis=0)
    padded_values = jnp.concatenate([margin, self_value, margin], axis=0)
    text_keys = text_key.astype(jnp.float32).reshape(TEXT, HEADS, HEAD_DIM)
    text_values = text_value.astype(jnp.float32).reshape(TEXT, HEADS, HEAD_DIM)
    text_usable = jnp.ones((TEXT,), dtype=bool)
    gate_row = lax.dynamic_slice_in_dim(gate_table, timestep[0].astype(jnp.int32), 1, 0).astype(jnp.float32)

    def one_tile(tile_index):
        start = (tile_index * TOK_DEV).astype(jnp.int32)
        queries = lax.dynamic_slice_in_dim(self_query, start, TOK_DEV, 0).astype(jnp.float32).reshape(TOK_DEV, HEADS, HEAD_DIM)
        key_block = lax.dynamic_slice_in_dim(padded_keys, start, window_span * TOK_DEV, 0).astype(jnp.float32).reshape(window_span * TOK_DEV, HEADS, HEAD_DIM)
        value_block = lax.dynamic_slice_in_dim(padded_values, start, window_span * TOK_DEV, 0).astype(jnp.float32).reshape(window_span * TOK_DEV, HEADS, HEAD_DIM)
        offsets = jnp.arange(window_span, dtype=jnp.int32) - RADIUS
        position = tile_index + offsets
        tile_usable = (position >= 0) & (position < TILES)
        usable = jnp.repeat(tile_usable, TOK_DEV)
        self_out = window_attention(queries, key_block, value_block, usable).reshape(TOK_DEV, width)
        cross_rows = lax.dynamic_slice_in_dim(cross_query, start, TOK_DEV, 0).astype(jnp.float32).reshape(TOK_DEV, HEADS, HEAD_DIM)
        cross_out = window_attention(cross_rows, text_keys, text_values, text_usable).reshape(TOK_DEV, width)
        return (gate_row * self_out + cross_out).astype(jnp.bfloat16)
    mixed = lax.map(one_tile, jnp.arange(TILES, dtype=jnp.int32))
    return mixed.reshape(TOKENS, width)
```

```python
import functools
import math

import jax
import jax.numpy as jnp
from jax import lax
from jax.experimental import pallas as pl
from jax.experimental.pallas import tpu as pltpu
from jax.sharding import PartitionSpec as P

HEADS = 32
RADIUS = 2
SPAN = 2 * RADIUS + 1
OWN = RADIUS
STEP_NUM, STEP_DEN = 3, 2
RECV_LAG, ATTEND_LAG = 2, 1
NEG = -1e30


def softmax_parts(scores, scale):
    top = jnp.max(scores, axis=1, keepdims=True)
    weights = jnp.exp2((scores - top) * (scale * math.log2(math.e)))
    return weights.astype(jnp.bfloat16), jnp.sum(weights, axis=1, keepdims=True)


def dot(a, b, contract_b):
    return lax.dot_general(a, b, (((1,), (contract_b,)), ((), ())), preferred_element_type=jnp.float32)


def kernel(
    tiles,
    step_ref, self_query, self_key, self_value, cross_query, text_key, text_value, gate_table,
    mixed,
    win, text, query_s, query_c, gates, gate, bias, acc, result,
    own_sem, load_sem,
    up_recv, down_recv, pair_recv, pass_recv, text_recv, text_pair_recv,
    text_sent, send_sem, out_sem,
):
    rows, width = query_s.shape
    dim = width // HEADS
    text_rows = text_key.shape[0]
    scale = 1.0 / math.sqrt(dim)
    chips = tiles // 2
    hops_up = chips // 2
    hops_down = chips - 1 - hops_up

    me = lax.axis_index("tile")
    core = lax.rem(me, 2)
    chip = lax.div(me, 2)
    above = lax.rem(me + 2, tiles)
    below = lax.rem(me + tiles - 2, tiles)
    partner = me + 1 - 2 * core
    has_below = chip > 0
    has_above = chip < chips - 1
    pair_slot = 1 + 2 * core
    pass_src = 4 - 4 * core
    pass_slot = 3 - 2 * core
    sends_pass = jnp.logical_or(jnp.logical_and(core == 1, has_below), jnp.logical_and(core == 0, has_above))
    gets_pass = jnp.logical_or(jnp.logical_and(core == 0, has_below), jnp.logical_and(core == 1, has_above))

    def remote(src, dst, which, recv, target):
        return pltpu.make_async_remote_copy(
            src_ref=src, dst_ref=dst, send_sem=send_sem.at[which], recv_sem=recv,
            device_id={"tile": target}, device_id_type=pl.DeviceIdType.MESH,
        )

    def columns(head):
        return pl.ds(pl.multiple_of(head * dim, dim), dim)

    def block(slot):
        return text.at[:, pl.ds(pl.multiple_of(slot * text_rows, text_rows), text_rows)]

    loads = [
        pltpu.make_async_copy(text_key, text.at[0, pl.ds(0, text_rows)], load_sem.at[0]),
        pltpu.make_async_copy(text_value, text.at[1, pl.ds(0, text_rows)], load_sem.at[1]),
        pltpu.make_async_copy(self_query, query_s, load_sem.at[2]),
        pltpu.make_async_copy(gate_table, gates, load_sem.at[3]),
        pltpu.make_async_copy(cross_query, query_c, load_sem.at[4]),
    ]

    def load_head(head):
        for which, source in enumerate((self_key, self_value)):
            pltpu.make_async_copy(source.at[:, columns(head)], win.at[OWN, head, which], own_sem.at[head]).start()

    def load_heads(first, last):
        lax.fori_loop(first, last, lambda head, c: (load_head(head), c)[1], 0)

    loads[0].start()
    loads[1].start()
    load_heads(0, 4)
    loads[2].start()
    load_heads(4, HEADS)
    loads[3].start()
    loads[4].start()

    barrier = pltpu.get_barrier_semaphore()
    for neighbour in (above, below, partner):
        pl.semaphore_signal(barrier, inc=1, device_id={"tile": neighbour}, device_id_type=pl.DeviceIdType.MESH)
    pl.semaphore_wait(barrier, 3)

    def head_copies(head):
        own = win.at[OWN, head]
        return (
            remote(own, win.at[0, head], 0, up_recv.at[head], above),
            remote(own, win.at[SPAN - 1, head], 1, down_recv.at[head], below),
            remote(own, win.at[pair_slot, head], 2, pair_recv.at[head], partner),
        )

    def pass_copy(head):
        return remote(win.at[pass_src, head], win.at[pass_slot, head], 3, pass_recv.at[head], partner)

    def send_head(head, carry):
        pltpu.make_async_copy(win.at[OWN, head], win.at[OWN, head], own_sem.at[head]).wait()
        up, down, pair = head_copies(head)

        @pl.when(has_above)
        def _():
            up.start()

        @pl.when(has_below)
        def _():
            down.start()

        pair.start()
        return carry

    def take_head(head, carry):
        up, down, _ = head_copies(head)

        @pl.when(has_below)
        def _():
            up.wait_recv()

        @pl.when(has_above)
        def _():
            down.wait_recv()

        @pl.when(sends_pass)
        def _():
            pass_copy(head).start()

        return carry

    def self_attend(head, write):
        pair = head_copies(head)[2]
        pair.wait_recv()

        @pl.when(gets_pass)
        def _():
            pass_copy(head).wait_recv()

        query = query_s[:, columns(head)]
        keys = win[:, head, 0].reshape(SPAN * rows, dim)
        values = win[:, head, 1].reshape(SPAN * rows, dim)
        weights, total = softmax_parts(dot(query, keys, 1) + bias[...], scale)
        attended = dot(weights, values, 0) / total
        mix(head, gate[:, columns(head)] * attended, write)

    def cross_attend(head, write):
        query = query_c[:, columns(head)]
        weights, total = softmax_parts(dot(query, text[0, :, columns(head)], 1), scale)
        mix(head, dot(weights, text[1, :, columns(head)], 0) / total, write)

    def out_copy(head):
        return pltpu.make_async_copy(result.at[:, columns(head)], mixed.at[:, columns(head)], out_sem)

    def mix(head, term, write):
        total = acc[:, columns(head)] + term
        acc[:, columns(head)] = total

        @pl.when(write)
        def _():
            result[:, columns(head)] = total.astype(result.dtype)
            out_copy(head).start()

    def text_copy(src, dst, target):
        return pltpu.make_async_remote_copy(
            src_ref=block(src), dst_ref=block(dst), send_sem=text_sent.at[dst], recv_sem=text_recv.at[dst],
            device_id={"tile": target}, device_id_type=pl.DeviceIdType.MESH,
        )

    def text_pair(slot):
        return remote(block(slot), block(chips + slot), 4, text_pair_recv.at[slot], partner)

    def sent_by(step):
        return jnp.minimum((STEP_NUM * (step + 1)) // STEP_DEN, HEADS) if not isinstance(step, int) else (
            min(max((STEP_NUM * (step + 1)) // STEP_DEN, 0), HEADS))

    def ring_step(step, carry):
        up_slot = step
        down_slot = jnp.where(step == 0, 0, hops_up + step)

        @pl.when(step > 0)
        def _():
            text_copy(0, up_slot, above).wait_recv()

        text_copy(up_slot, step + 1, above).start()

        @pl.when(jnp.logical_and(step > 0, step <= hops_down))
        def _():
            text_copy(0, down_slot, below).wait_recv()

        @pl.when(step < hops_down)
        def _():
            text_copy(down_slot, hops_up + step + 1, below).start()

        lax.fori_loop(sent_by(step - 1), sent_by(step), send_head, 0)
        text_pair(up_slot).start()

        @pl.when(jnp.logical_and(step > 0, step <= hops_down))
        def _():
            text_pair(down_slot).start()

        @pl.when(step == 0)
        def _():
            prepare()

        @pl.when(step >= RECV_LAG)
        def _():
            lax.fori_loop(sent_by(step - RECV_LAG - 1), sent_by(step - RECV_LAG), take_head, 0)

        lag = RECV_LAG + ATTEND_LAG

        @pl.when(step >= lag)
        def _():
            lax.fori_loop(sent_by(step - lag - 1), sent_by(step - lag), attend_only, 0)

        return carry

    def attend_only(head, carry):
        self_attend(head, False)
        return carry

    def prepare():
        usable = (has_below, jnp.logical_or(core == 1, has_below), None, jnp.logical_or(core == 0, has_above), has_above)
        for slot in range(SPAN):
            here = pl.ds(slot * rows, rows)
            if usable[slot] is None:
                bias[:, here] = jnp.zeros((1, rows), jnp.float32)
                continue
            bias[:, here] = jnp.full((1, rows), jnp.where(usable[slot], 0.0, NEG), jnp.float32)

            @pl.when(jnp.logical_not(usable[slot]))
            def _(slot=slot):
                def clear(head, c):
                    win[slot, head] = jnp.zeros(win.shape[2:], win.dtype)
                    return c

                lax.fori_loop(0, HEADS, clear, 0)

        def clear_acc(head, c):
            acc[:, columns(head)] = jnp.zeros((rows, dim), jnp.float32)
            return c

        lax.fori_loop(0, HEADS, clear_acc, 0)
        loads[2].wait()
        loads[3].wait()
        loads[4].wait()
        picked = lax.broadcasted_iota(jnp.int32, (gates.shape[0], dim), 0) == step_ref[0]

        def pick(head, c):
            table = gates[:, columns(head)].astype(jnp.float32)
            gate[:, columns(head)] = jnp.sum(jnp.where(picked, table, 0.0), axis=0, keepdims=True)
            return c

        lax.fori_loop(0, HEADS, pick, 0)

    loads[0].wait()
    loads[1].wait()
    lax.fori_loop(0, hops_up, ring_step, 0)

    sent = sent_by(hops_up - 1)
    taken = sent_by(hops_up - 1 - RECV_LAG) if hops_up > RECV_LAG else 0
    attended = sent_by(hops_up - 1 - RECV_LAG - ATTEND_LAG) if hops_up > RECV_LAG + ATTEND_LAG else 0
    lax.fori_loop(sent, HEADS, send_head, 0)
    text_copy(0, hops_up, above).wait_recv()
    text_pair(hops_up).start()
    lax.fori_loop(attended, taken, attend_only, 0)

    def pair_wait(slot, carry):
        text_pair(slot).wait_recv()
        return carry

    steps = HEADS - taken
    each = -(-HEADS // steps)

    def tail_step(i, carry):
        take_head(taken + i, 0)

        @pl.when(i == 0)
        def _():
            lax.fori_loop(0, chips, pair_wait, 0)

        for k in range(each):
            index = i * each + k

            @pl.when(index < HEADS)
            def _(index=index):
                head = lax.rem(taken + index, HEADS)
                cross_attend(head, head < taken)

        @pl.when(i > 0)
        def _():
            self_attend(taken + i - 1, True)

        return carry

    lax.fori_loop(0, steps, tail_step, 0)
    self_attend(HEADS - 1, True)

    @pl.when(has_above)
    def _():
        remote(win.at[OWN], win.at[0], 0, up_recv.at[0], above).wait_send()

    @pl.when(has_below)
    def _():
        remote(win.at[OWN], win.at[SPAN - 1], 1, down_recv.at[0], below).wait_send()

    remote(win.at[OWN], win.at[pair_slot], 2, pair_recv.at[0], partner).wait_send()

    @pl.when(sends_pass)
    def _():
        remote(win.at[pass_src], win.at[pass_slot], 3, pass_recv.at[0], partner).wait_send()

    def text_gone(slot, carry):
        text_copy(0, slot, above).wait_send()
        return carry

    lax.fori_loop(1, chips, text_gone, 0)
    whole = text.at[:, pl.ds(0, chips * text_rows)]
    remote(whole, whole, 4, text_pair_recv.at[0], partner).wait_send()
    pltpu.make_async_copy(result, mixed, out_sem).wait()


def solution(mesh):
    tiles = mesh.shape["tile"]

    def shards(self_query, self_key, self_value, cross_query, text_key, text_value, timestep, gate_table):
        rows, width = self_query.shape
        dim = width // HEADS
        chips = tiles // 2
        text_rows = text_key.shape[0] * tiles
        bf16, f32 = jnp.bfloat16, jnp.float32
        dma = pltpu.SemaphoreType.DMA
        anywhere = pl.BlockSpec(memory_space=pl.ANY)
        return pl.pallas_call(
            functools.partial(kernel, tiles),
            name="window_attention",
            out_shape=jax.ShapeDtypeStruct((rows, width), bf16),
            in_specs=[pl.BlockSpec(memory_space=pltpu.SMEM)] + [anywhere] * 7,
            out_specs=anywhere,
            scratch_shapes=[
                pltpu.VMEM((SPAN, HEADS, 2, rows, dim), bf16),
                pltpu.VMEM((2, text_rows, width), bf16),
                pltpu.VMEM((rows, width), bf16),
                pltpu.VMEM((rows, width), bf16),
                pltpu.VMEM(gate_table.shape, bf16),
                pltpu.VMEM((1, width), f32),
                pltpu.VMEM((1, SPAN * rows), f32),
                pltpu.VMEM((rows, width), f32),
                pltpu.VMEM((rows, width), bf16),
                dma((HEADS,)),
                dma((5,)),
                dma((HEADS,)),
                dma((HEADS,)),
                dma((HEADS,)),
                dma((HEADS,)),
                dma((chips,)),
                dma((chips,)),
                dma((chips,)),
                dma((5,)),
                dma,
            ],
            compiler_params=pltpu.CompilerParams(collective_id=0, has_side_effects=True),
        )(timestep, self_query, self_key, self_value, cross_query, text_key, text_value, gate_table)

    rowwise = P(("groups", "tile"), None)
    return jax.shard_map(
        shards, mesh=mesh, in_specs=(rowwise,) * 6 + (P(), P()), out_specs=rowwise, check_vma=False
    )
```
